256 devices in a mesh: dp: 8 (over z), vocab: 32 (over x, y, core).
Axes of the slice: x: 4, y: 4, z: 8, core: 2. Of those that a mesh axis runs over, the one named last changes fastest.
Arguments:
- token_ids: int32 [65536], P(('dp', 'vocab')), may hold values from 0 to 152063, as said below
- token_count: int32 [256], P(('dp', 'vocab')), may hold values from 16 to 256
- out_grads: bfloat16 [65536, 5120], P(('dp', 'vocab')), may hold values from -18 to 18
- master_rows: float32 [16384, 5120], P('vocab', 'dp'), may hold values from -0.8 to 0.8
- first_moment: float32 [16384, 5120], P('vocab', 'dp'), may hold values from -4 to 4
- second_moment: float32 [16384, 5120], P('vocab', 'dp'), may hold values from 0.001 to 1
Outputs:
- new_master: float32 [16384, 5120], P('vocab', 'dp')
- new_first: float32 [16384, 5120], P('vocab', 'dp')
- new_second: float32 [16384, 5120], P('vocab', 'dp')
- table_rows: bfloat16 [16384, 5120], P('vocab')
The draws below stay inside these ranges and needn't reach their ends.
Inputs may be any that keep to these rules, and one draw needn't show every extreme that they name: `token_ids`: within each block of 256 slots, among the live slots (the first token_count of the block) at most 8 have ids in the new rows j * 512 + 135680 to (j + 1) * 512 + 135679 for any one j, and for some j exactly 8 in every block. Slots past token_count hold ids of new rows that are to be ignored.
All inputs are finite; a program needn't handle non-finite values.
Results may differ from the reference program's by a relative error of at most 0.001.
Values may be sent and summed in bfloat16 or wider, within the bound.
No kernel may reach another device: no remote copies, remote signals or barrier semaphores. Data moves between devices by JAX's collectives and lax.ppermute only.
A program may use at most 64 MiB of HBM per device.

```python
import math
import jax
import jax.numpy as jnp
from jax import lax

D = 5120
VOCAB = 152064
T_DEV = 256
NEW_DEV = 512
CAP = 8
NEW = 16384
TOKENS = 65536


def layout_tokens(key):
    key = jax.random.fold_in(key, 7)
    owners = NEW // NEW_DEV
    blocks = TOKENS // T_DEV
    keys = jax.random.split(key, 7)
    hottest = jax.random.randint(keys[0], (2,), 0, owners)
    baseline = jax.random.randint(keys[1], (blocks, owners), 0, CAP + 1)
    owner_axis = jnp.arange(owners)
    is_hot = (owner_axis[None, :] == hottest[0]) | (owner_axis[None, :] == hottest[1])
    per_owner = jnp.where(is_hot, CAP, baseline)
    ends = jnp.cumsum(per_owner, axis=1)
    new_total = ends[:, -1]
    extra = jax.random.randint(keys[2], (blocks,), 0, 1 << 20)
    live_count = new_total + extra % (T_DEV - new_total + 1)
    slots = jnp.arange(T_DEV)
    owner_of = jnp.sum((slots[None, :, None] >= ends[:, None, :]).astype(jnp.int32), axis=2)
    owner_of = jnp.minimum(owner_of, owners - 1)
    is_new = slots[None, :] < new_total[:, None]
    row_pick = jax.random.randint(keys[3], (blocks, T_DEV), 0, NEW_DEV)
    new_ids = VOCAB - NEW + owner_of * NEW_DEV + row_pick
    old_ids = jax.random.randint(keys[4], (blocks, T_DEV), 0, VOCAB - NEW)
    pad_ids = jax.random.randint(keys[5], (blocks, T_DEV), VOCAB - NEW, VOCAB)
    ordered = jnp.where(is_new, new_ids, old_ids)
    scores = jax.random.randint(keys[6], (blocks, T_DEV), 0, 1 << 20)
    is_head = slots[None, :] < live_count[:, None]
    keyed = jnp.where(is_head, scores * T_DEV + slots[None, :], (1 << 20) * T_DEV + slots[None, :])
    order = jnp.argsort(keyed, axis=1)
    shuffled = jnp.take_along_axis(ordered, order, axis=1)
    final_ids = jnp.where(is_head, shuffled, pad_ids)
    return (final_ids.reshape(TOKENS).astype(jnp.int32), live_count.astype(jnp.int32))


def draw_token_ids(key, part):
    return layout_tokens(key)[0]


def draw_token_count(key, part):
    return layout_tokens(key)[1]


def levels(stream_key, extent, pieces, smallest, largest):
    gain, own = 1.0, jax.random.fold_in(stream_key, 6)
    for axis_at, shards_of in pieces:
        steps = jnp.exp(jax.random.uniform(jax.random.fold_in(own, axis_at), (shards_of,), jnp.float32, smallest / len(pieces), largest / len(pieces)))
        gain = gain * jnp.repeat(steps, extent[axis_at] // shards_of).reshape([-1 if axis == axis_at else 1 for axis in range(len(extent))])
    return gain


def centred(stream_key, shape, width, most, pieces=(), held_as=jnp.bfloat16):
    level = levels(stream_key, shape, pieces, -0.22, 0.18) if pieces else 1.0
    entries = jax.random.normal(stream_key, shape, jnp.float32) * width * level
    return jnp.minimum(jnp.maximum(entries, -most), most).astype(held_as)


def setup_inputs(seed: int = 0) -> dict:
    seeds = jax.random.split(jax.random.key(seed), 7)
    return {
        "token_ids": draw_token_ids(jax.random.fold_in(seeds[6], 71), 0),
        "token_count": draw_token_count(jax.random.fold_in(seeds[6], 71), 0),
        "out_grads": centred(seeds[2], (TOKENS, D), 3.0, 18.0, ((0, 256),)),
        "master_rows": centred(seeds[3], (NEW, D), 0.2, 0.8, ((0, 32), (1, 8)), jnp.float32),
        "first_moment": centred(seeds[4], (NEW, D), 0.5, 4.0, ((0, 32), (1, 8)), jnp.float32),
        "second_moment": jnp.clip(jnp.exp(math.log(1.0) - 6.9077552 * jax.random.uniform(seeds[5], (NEW, D), jnp.float32) ** levels(seeds[5], (NEW, D), ((0, 32), (1, 8)), -0.2, 0.2)), 0.001, 1.0),
    }


beta_one = 0.9
beta_two = 0.999
corr_one = 1.0 - 0.9 ** 10
corr_two = 1.0 - 0.999 ** 10
learn_rate = 0.01
epsilon = 1e-08

def reference(token_ids, token_count, out_grads, master_rows, first_moment, second_moment):
    first_new = VOCAB - NEW
    blocks = token_ids.shape[0] // T_DEV
    ids_blocks = token_ids.reshape(blocks, T_DEV)
    position = jnp.arange(T_DEV)
    is_live = (position[None, :] < token_count[:, None]) & (ids_blocks >= first_new)
    segment = jnp.where(is_live, ids_blocks - first_new, NEW)
    grad_blocks = out_grads.reshape(blocks, T_DEV, D)

    def add_block(running, inputs):
        ids_block, grad_block = inputs
        summed = jax.ops.segment_sum(grad_block.astype(jnp.float32), ids_block, num_segments=NEW + 1)
        return (running + summed, None)
    grad_all, _ = lax.scan(add_block, jnp.zeros((NEW + 1, D), jnp.float32), (segment, grad_blocks))
    gradient = grad_all[:NEW]
    new_first = beta_one * first_moment + (1.0 - beta_one) * gradient
    new_second = beta_two * second_moment + (1.0 - beta_two) * gradient * gradient
    update = new_first / corr_one / (jnp.sqrt(new_second / corr_two) + epsilon)
    new_master = master_rows - learn_rate * update
    return (new_master, new_first, new_second, new_master.astype(jnp.bfloat16))
```

```python
import jax
import jax.numpy as jnp
from jax import lax
from jax.experimental import pallas as pl
from jax.experimental.pallas import tpu as pltpu
from jax.sharding import PartitionSpec as P

VOCAB = 152064
CAP = 8

beta_one = 0.9
beta_two = 0.999
corr_one = 1.0 - 0.9**10
corr_two = 1.0 - 0.999**10
learn_rate = 0.01
epsilon = 1e-08


CHUNK_ONE = 256
EMPTY = 2048.0
META_ROWS = 8


def smem():
    return pl.BlockSpec(memory_space=pltpu.SMEM)


def anywhere():
    return pl.BlockSpec(memory_space=pl.ANY)


def prep_kernel(where_ref, count_ref, ids_ref, grads_ref, first_ref, *second_refs, owners, groups, rows_own, cols, cut):
    slots = ids_ref.shape[1]
    first_new = VOCAB - rows_own * owners
    z = where_ref[0]
    ids = ids_ref[...]
    position = lax.broadcasted_iota(jnp.int32, (1, slots), 1)
    live = (position < count_ref[0]) & (ids >= first_new)
    index = ids - first_new
    owner = index // rows_own
    row = index - owner * rows_own
    key = jnp.where(live, owner, -1)
    key_row = jnp.broadcast_to(key, (slots, slots))
    key_col = key_row.T
    lane = lax.broadcasted_iota(jnp.int32, (slots, slots), 1)
    sub = lax.broadcasted_iota(jnp.int32, (slots, slots), 0)
    earlier = (key_row == key_col) & (sub < lane)
    rank = jnp.sum(earlier.astype(jnp.int32), axis=0, keepdims=True)
    place = jnp.where(live, owner * CAP + rank, -1)
    place_row = jnp.broadcast_to(place, (slots, slots))
    placing = (sub == place_row).astype(jnp.bfloat16)
    place_col = place_row.T
    row_col = jnp.broadcast_to(row, (slots, slots)).T
    code = jnp.where(place_col == lane, row_col + 1, 0)
    code = jnp.sum(code, axis=0, keepdims=True).astype(jnp.float32)
    code = jnp.where(code > 0.0, code - 1.0 - rows_own // 2, EMPTY)
    meta = jnp.broadcast_to(code, (META_ROWS, slots)).astype(jnp.bfloat16)
    for g in range(groups):
        at = pl.multiple_of(g * cols, 128)
        got = jnp.dot(placing, grads_ref[:, pl.ds(at, cut)], preferred_element_type=jnp.float32)
        first_ref[g, :slots, :] = got.astype(jnp.bfloat16)
        first_ref[g, slots:, :slots] = meta
    for k in range(groups):
        g = lax.rem(z + k, groups)
        at = pl.multiple_of(g * cols + cut, 128)
        got = jnp.dot(placing, grads_ref[:, pl.ds(at, cols - cut)], preferred_element_type=jnp.float32)
        second_refs[k][...] = got.astype(jnp.bfloat16)


def weave_one_kernel(in_ref, out_ref, *, owners, groups):
    slots = owners * CAP
    meta = in_ref[:, slots, :]
    for o in range(owners):
        for g in range(groups):
            out_ref[o, g * CAP : (g + 1) * CAP, :] = in_ref[g, o * CAP : (o + 1) * CAP, :]
        out_ref[o, groups * CAP :, :] = meta


def weave_two_kernel(*refs, owners, groups):
    out_ref = refs[groups]
    for o in range(owners):
        for g in range(groups):
            out_ref[o, g * CAP : (g + 1) * CAP, :] = refs[g][o * CAP : (o + 1) * CAP, :]


def adam(gradient, first, second, master):
    new_first = beta_one * first + (1.0 - beta_one) * gradient
    new_second = beta_two * second + (1.0 - beta_two) * gradient * gradient
    update = new_first / corr_one / (jnp.sqrt(new_second / corr_two) + epsilon)
    return new_first, new_second, master - learn_rate * update


def gradient_of(tokens_ref, meta_rows, owners, groups, rows_own):
    width = tokens_ref.shape[2]
    total = None
    for g in range(groups):
        ids = jnp.broadcast_to(meta_rows[g], (rows_own, owners * CAP))
        sub = lax.broadcasted_iota(jnp.int32, ids.shape, 0).astype(jnp.float32) - float(rows_own // 2)
        selector = (sub == ids).astype(jnp.bfloat16)
        data = tokens_ref[:, g * CAP : (g + 1) * CAP, :].reshape(owners * CAP, width)
        part = jnp.dot(selector, data, preferred_element_type=jnp.float32)
        total = part if total is None else total + part
    return total


def step_one_kernel(where_ref, tokens_ref, master_ref, first_ref, second_ref, *outs, owners, groups, cut):
    om_ref, of_ref, os_ref, piece_ref, meta_ref = outs
    rows_own = master_ref.shape[0]
    slots = owners * CAP
    mine = where_ref[1]
    lane = lax.broadcasted_iota(jnp.int32, (groups, slots), 1)
    meta = jnp.zeros((groups, slots), jnp.float32)
    for v in range(owners):
        got = tokens_ref[v, groups * CAP :, :slots].astype(jnp.float32)
        shift = lax.rem((v + owners - mine) * CAP, slots)
        got = pltpu.roll(got, shift, 1)
        meta = jnp.where(lane // CAP == v, got, meta)
    meta_ref[...] = meta
    gradient = gradient_of(tokens_ref, [meta[g : g + 1, :] for g in range(groups)], owners, groups, rows_own)
    new_first, new_second, new_master = adam(gradient, first_ref[:, :cut], second_ref[:, :cut], master_ref[:, :cut])
    om_ref[:, :cut] = new_master
    of_ref[:, :cut] = new_first
    os_ref[:, :cut] = new_second
    piece_ref[...] = new_master.astype(jnp.bfloat16)


def step_two_kernel(
    where_ref, tokens_ref, meta_ref, master_ref, first_ref, second_ref, am_ref, af_ref, as_ref, *outs, owners, groups, cut, widths
):
    om_ref, of_ref, os_ref = outs[:3]
    rows_own = master_ref.shape[0]
    z = where_ref[0]
    rows = [meta_ref[pl.ds(lax.rem(z + groups - k, groups), 1), :] for k in range(groups)]
    gradient = gradient_of(tokens_ref, rows, owners, groups, rows_own)
    new_first, new_second, new_master = adam(gradient, first_ref[:, cut:], second_ref[:, cut:], master_ref[:, cut:])
    om_ref[:, :cut] = am_ref[:, :cut]
    of_ref[:, :cut] = af_ref[:, :cut]
    os_ref[:, :cut] = as_ref[:, :cut]
    om_ref[:, cut:] = new_master
    of_ref[:, cut:] = new_first
    os_ref[:, cut:] = new_second
    rounded = new_master.astype(jnp.bfloat16)
    at = 0
    for piece_ref, width in zip(outs[3:], widths):
        piece_ref[...] = rounded[:, at : at + width]
        at += width


def put_kernel(where_ref, *refs, spots, cols, groups, aliased):
    count = len(spots)
    ins = refs[:count]
    table_ref = refs[count + (1 if aliased else 0)]
    sem = refs[-1]
    z = where_ref[0]
    copies = []
    for i, (shift, row, off) in enumerate(spots):
        n, w = ins[i].shape
        g = lax.rem(z + groups - shift, groups)
        at = pl.multiple_of(g * cols + off, 128)
        copies.append(pltpu.make_async_copy(ins[i], table_ref.at[pl.ds(row, n), pl.ds(at, w)], sem.at[i]))
    for c in copies:
        c.start()
    for c in copies:
        c.wait()


def put(table, where, pieces, shape, cols, groups):
    arrays = [p[0] for p in pieces]
    spots = tuple(p[1:] for p in pieces)
    aliased = table is not None
    extra = [table] if aliased else []
    import functools

    return pl.pallas_call(
        functools.partial(put_kernel, spots=spots, cols=cols, groups=groups, aliased=aliased),
        out_shape=jax.ShapeDtypeStruct(shape, jnp.bfloat16),
        in_specs=[smem()] + [anywhere() for _ in arrays + extra],
        out_specs=anywhere(),
        input_output_aliases={len(arrays) + 1: 0} if aliased else {},
        scratch_shapes=[pltpu.SemaphoreType.DMA((len(arrays),))],
        name="put",
    )(where, *arrays, *extra)


def shift_by(x, k, groups):
    return lax.ppermute(x, "dp", [(i, (i + k) % groups) for i in range(groups)])


def ring(piece, off, groups):
    half = groups // 2
    rows = piece.shape[0]
    got = [(piece, 0, 0, off)]
    up = down = piece
    for s in range(1, half):
        up = shift_by(up, 1, groups)
        down = shift_by(down, -1, groups)
        got += [(up, s, 0, off), (down, groups - s, 0, off)]
    last = [
        (shift_by(up[: rows // 2], 1, groups), half, 0, off),
        (shift_by(down[rows // 2 :], -1, groups), half, rows // 2, off),
    ]
    return got, last


def body(token_ids, token_count, out_grads, master_rows, first_moment, second_moment):
    import functools

    owners = lax.axis_size("vocab")
    groups = lax.axis_size("dp")
    rows_own, cols = master_rows.shape
    slots = token_ids.shape[0]
    cut = CHUNK_ONE
    rest = cols - cut
    bf16 = jnp.bfloat16
    where = jnp.stack([lax.axis_index("dp"), lax.axis_index("vocab")]).astype(jnp.int32)
    outs = pl.pallas_call(
        functools.partial(prep_kernel, owners=owners, groups=groups, rows_own=rows_own, cols=cols, cut=cut),
        out_shape=[jax.ShapeDtypeStruct((groups, slots + META_ROWS, cut), bf16)]
        + [jax.ShapeDtypeStruct((slots, rest), bf16) for _ in range(groups)],
        in_specs=[smem(), smem(), pl.BlockSpec(), pl.BlockSpec()],
        name="prep",
    )(where, token_count, token_ids.reshape(1, slots), out_grads)
    one = lax.all_to_all(outs[0], "dp", split_axis=0, concat_axis=0, tiled=True)
    two = [outs[1]] + [shift_by(outs[1 + k], k, groups) for k in range(1, groups)]
    woven = pl.pallas_call(
        functools.partial(weave_one_kernel, owners=owners, groups=groups),
        out_shape=jax.ShapeDtypeStruct((owners, groups * CAP + META_ROWS, cut), bf16),
        name="weave_one",
    )(one)
    tokens_one = lax.all_to_all(woven, "vocab", split_axis=0, concat_axis=0, tiled=True)
    state = jax.ShapeDtypeStruct((rows_own, cols), jnp.float32)
    vm = pl.BlockSpec()
    om, of, os, piece_one, meta = pl.pallas_call(
        functools.partial(step_one_kernel, owners=owners, groups=groups, cut=cut),
        out_shape=[state, state, state, jax.ShapeDtypeStruct((rows_own, cut), bf16), jax.ShapeDtypeStruct((groups, slots), jnp.float32)],
        in_specs=[smem(), vm, vm, vm, vm],
        name="step_one",
    )(where, tokens_one, master_rows, first_moment, second_moment)
    got_one, last_one = ring(piece_one, 0, groups)
    woven_two = pl.pallas_call(
        functools.partial(weave_two_kernel, owners=owners, groups=groups),
        out_shape=jax.ShapeDtypeStruct((owners, groups * CAP, rest), bf16),
        name="weave_two",
    )(*two)
    tokens_two = lax.all_to_all(woven_two, "vocab", split_axis=0, concat_axis=0, tiled=True)
    widths = (256, rest - 256)
    om, of, os, *pieces = pl.pallas_call(
        functools.partial(step_two_kernel, owners=owners, groups=groups, cut=cut, widths=widths),
        out_shape=[state, state, state] + [jax.ShapeDtypeStruct((rows_own, w), bf16) for w in widths],
        in_specs=[smem()] + [vm] * 8,
        input_output_aliases={6: 0, 7: 1, 8: 2},
        name="step_two",
    )(where, tokens_two, meta, master_rows, first_moment, second_moment, om, of, os)
    shape = (rows_own, cols * groups)
    table = put(None, where, got_one + last_one, shape, cols, groups)
    got_a, last_a = ring(pieces[0], cut, groups)
    got_b, last_b = ring(pieces[1], cut + widths[0], groups)
    table = put(table, where, got_a + got_b, shape, cols, groups)
    table = put(table, where, last_a + last_b, shape, cols, groups)
    return (om, of, os, table)


def solution(mesh):
    return jax.shard_map(
        body,
        mesh=mesh,
        in_specs=(
            P(("dp", "vocab")),
            P(("dp", "vocab")),
            P(("dp", "vocab"), None),
            P("vocab", "dp"),
            P("vocab", "dp"),
            P("vocab", "dp"),
        ),
        out_specs=(P("vocab", "dp"), P("vocab", "dp"), P("vocab", "dp"), P("vocab", None)),
        check_vma=False,
    )
```

```python
import functools

import jax
import jax.numpy as jnp
from jax import lax
from jax.experimental import pallas as pl
from jax.experimental.pallas import tpu as pltpu
from jax.sharding import PartitionSpec as P


VOCAB = 152064
CAP = 8

beta_one = 0.9
beta_two = 0.999
corr_one = 1.0 - 0.9**10
corr_two = 1.0 - 0.999**10
learn_rate = 0.01
epsilon = 1e-08


def near(x):
    return pltpu.with_memory_space_constraint(x, pltpu.VMEM)


def far(x):
    return pltpu.with_memory_space_constraint(x, pltpu.HBM)


SM = pl.BlockSpec(memory_space=pltpu.SMEM)
VM = pl.BlockSpec(memory_space=pltpu.VMEM)
HB = pl.BlockSpec(memory_space=pltpu.HBM)


def kernel(fn, out_shape, in_specs, out_specs, vmem_limit=24 << 20, **kw):
    def call(*args):
        return pl.pallas_call(
            fn,
            out_shape=out_shape,
            in_specs=in_specs,
            out_specs=out_specs,
            compiler_params=pltpu.CompilerParams(vmem_limit_bytes=vmem_limit),
            **kw,
        )(*args)

    return call


def prep_kernel(count_ref, ids_ref, grads_ref, out_ref, local_ref, buf, sems, *, owners, groups, rows_own, cols):
    slots = ids_ref.shape[1]
    copies = [pltpu.make_async_copy(grads_ref.at[:, g * cols : (g + 1) * cols], buf.at[g], sems.at[g]) for g in range(groups)]
    for c in copies:
        c.start()
    first_new = VOCAB - rows_own * owners
    ids = ids_ref[...]
    position = lax.broadcasted_iota(jnp.int32, (1, slots), 1)
    live = (position < count_ref[0]) & (ids >= first_new)
    local = jnp.where(live, ids - first_new, -1)
    local_ref[...] = local
    owner = jnp.where(live, local // rows_own, -1)
    key_row = jnp.broadcast_to(owner, (slots, slots))
    key_col = key_row.T
    lane = lax.broadcasted_iota(jnp.int32, (slots, slots), 1)
    sub = lax.broadcasted_iota(jnp.int32, (slots, slots), 0)
    earlier = (key_row == key_col) & (sub < lane)
    rank = jnp.sum(earlier.astype(jnp.int32), axis=0, keepdims=True)
    place = jnp.where(live, owner * CAP + rank, -1)
    placing = (sub == jnp.broadcast_to(place, (slots, slots))).astype(jnp.bfloat16)
    for g in range(groups):
        copies[g].wait()
        got = jnp.dot(placing, buf[g], preferred_element_type=jnp.float32).astype(jnp.bfloat16)
        out_ref[g * owners : (g + 1) * owners] = got.reshape(owners, CAP, cols)


def rows_kernel(mine_ref, local_ref, out_ref, *, rows_own):
    owners, slots = local_ref.shape
    mine = mine_ref[0]
    local = local_ref[...]
    here = (local >= mine * rows_own) & (local < (mine + 1) * rows_own)
    row = jnp.where(here, local - mine * rows_own, 0)
    sub = lax.broadcasted_iota(jnp.int32, (slots, slots), 0)
    lane = lax.broadcasted_iota(jnp.int32, (slots, slots), 1)
    ahead = (sub < lane).astype(jnp.bfloat16)
    rank = jnp.dot(here.astype(jnp.bfloat16), ahead, preferred_element_type=jnp.float32)
    lanes = lax.broadcasted_iota(jnp.int32, (owners, slots), 1)
    total = jnp.zeros((owners, slots), jnp.int32)
    for s in range(CAP):
        picked = jnp.where(here & (rank == float(s)), row + 1, 0)
        total = jnp.where(lax.rem(lanes, CAP) == s, jnp.sum(picked, axis=1, keepdims=True), total)
    source = lax.broadcasted_iota(jnp.int32, (owners, slots), 0) ^ mine
    codes = jnp.sum(jnp.where(lanes // CAP == source, total, 0), axis=0, keepdims=True) - 1
    out_ref[...] = jnp.broadcast_to(codes, out_ref.shape)


def adam(gradient, first, second, master):
    new_first = beta_one * first + (1.0 - beta_one) * gradient
    new_second = beta_two * second + (1.0 - beta_two) * gradient * gradient
    update = new_first / corr_one / (jnp.sqrt(new_second / corr_two) + epsilon)
    return new_first, new_second, master - learn_rate * update


def adam_kernel(where_ref, tokens_ref, *refs, owners, groups, at, width, pieces, aliased):
    codes, refs = refs[:groups], refs[groups:]
    state, refs = refs[:3], refs[3 + (3 if aliased else 0) :]
    outs, refs = refs[:3], refs[3:]
    piece_refs, refs = refs[: len(pieces)], refs[len(pieces) :]
    code_buf, b0, b1, b2, sems = refs
    bufs = (b0, b1, b2)
    into = [pltpu.make_async_copy(r.at[:, pl.ds(at, width)], b, sems.at[i]) for i, (r, b) in enumerate(zip(state, bufs))]
    for c in into:
        c.start()
    rows_own = b0.shape[0]
    slots = owners * CAP
    z = where_ref[0]
    for k in range(groups):
        code_buf[lax.rem(z + groups - k, groups)] = codes[k][...]
    sub = lax.broadcasted_iota(jnp.int32, (rows_own, slots), 0)
    gradient = None
    for g in range(groups):
        code = jnp.broadcast_to(code_buf[g, 0:1, :], (rows_own, slots))
        selector = (sub == code).astype(jnp.bfloat16)
        data = tokens_ref[g * owners : (g + 1) * owners, :, at : at + width].reshape(slots, width)
        part = jnp.dot(selector, data, preferred_element_type=jnp.float32)
        gradient = part if gradient is None else gradient + part
    for c in into:
        c.wait()
    new_first, new_second, new_master = adam(gradient, b1[...], b2[...], b0[...])
    rounded = new_master.astype(jnp.bfloat16)
    b0[...] = new_master
    b1[...] = new_first
    b2[...] = new_second
    out = [pltpu.make_async_copy(b, r.at[:, pl.ds(at, width)], sems.at[i]) for i, (r, b) in enumerate(zip(outs, bufs))]
    for c in out:
        c.start()
    done = 0
    for piece_ref, w in zip(piece_refs, pieces):
        piece_ref[...] = rounded[:, done : done + w]
        done += w
    for c in out:
        c.wait()


def put_kernel(where_ref, *refs, spots, cols, groups, aliased):
    count = len(spots)
    ins = refs[:count]
    table_ref = refs[count + (1 if aliased else 0)]
    sem = refs[-1]
    z = where_ref[0]
    copies = []
    for i, (shift, row, off) in enumerate(spots):
        n, w = ins[i].shape
        g = lax.rem(z + groups - shift, groups)
        at = pl.multiple_of(g * cols + off, 128)
        copies.append(pltpu.make_async_copy(ins[i], table_ref.at[pl.ds(row, n), pl.ds(at, w)], sem.at[i]))
    for c in copies:
        c.start()
    for c in copies:
        c.wait()


def put(table, where, pieces, shape, cols, groups):
    arrays = [near(p[0]) for p in pieces]
    spots = tuple(p[1:] for p in pieces)
    aliased = table is not None
    extra = [far(table)] if aliased else []
    return kernel(
        functools.partial(put_kernel, spots=spots, cols=cols, groups=groups, aliased=aliased),
        jax.ShapeDtypeStruct(shape, jnp.bfloat16),
        [SM] + [VM for _ in arrays] + [HB for _ in extra],
        HB,
        input_output_aliases={len(arrays) + 1: 0} if aliased else {},
        scratch_shapes=[pltpu.SemaphoreType.DMA((len(arrays),))],
    )(where, *arrays, *extra)


def shift_by(x, k, groups):
    return lax.ppermute(x, "dp", [(i, (i + k) % groups) for i in range(groups)])


def ring(piece, off, groups):
    half = groups // 2
    rows = piece.shape[0]
    got = [(piece, 0, 0, off)]
    up = down = piece
    for s in range(1, half):
        up = shift_by(up, 1, groups)
        down = shift_by(down, -1, groups)
        got += [(up, s, 0, off), (down, groups - s, 0, off)]
    last = [
        (shift_by(up[: rows // 2], 1, groups), half, 0, off),
        (shift_by(down[rows // 2 :], -1, groups), half, rows // 2, off),
    ]
    return got, last


def step(token_ids, token_count, out_grads, master_rows, first_moment, second_moment):
    owners = lax.axis_size("vocab")
    groups = lax.axis_size("dp")
    rows_own, cols = master_rows.shape
    slots = token_ids.shape[0]
    bf16, i32 = jnp.bfloat16, jnp.int32
    z = lax.axis_index("dp").astype(i32).reshape(1)
    mine = lax.axis_index("vocab").astype(i32).reshape(1)
    sizes = dict(owners=owners, groups=groups)
    state = jax.ShapeDtypeStruct((rows_own, cols), jnp.float32)
    master_rows, first_moment, second_moment = far(master_rows), far(first_moment), far(second_moment)

    outgoing, local = kernel(
        functools.partial(prep_kernel, rows_own=rows_own, cols=cols, **sizes),
        [pltpu.VMEM((groups * owners, CAP, cols), bf16), pltpu.VMEM((1, slots), i32)],
        [SM, VM, HB],
        [VM, VM],
        scratch_shapes=[pltpu.VMEM((groups, slots, cols), bf16), pltpu.SemaphoreType.DMA((groups,))],
    )(token_count, token_ids.reshape(1, slots), far(out_grads))
    tokens = lax.all_to_all(outgoing, ("dp", "vocab"), split_axis=0, concat_axis=0, tiled=True)
    reach = 1
    while reach < owners:
        other = lax.ppermute(local, "vocab", [(i, i ^ reach) for i in range(owners)])
        local = jnp.concatenate([local, other], 0)
        reach *= 2
    codes = kernel(
        functools.partial(rows_kernel, rows_own=rows_own),
        jax.ShapeDtypeStruct((8, slots), i32),
        [SM, pl.BlockSpec()],
        pl.BlockSpec(),
    )(mine, local)
    codes = [codes] + [shift_by(codes, k, groups) for k in range(1, groups)]

    def adam_part(at, pieces, previous):
        width = sum(pieces)
        aliased = previous is not None
        n_in = 2 + groups + 3
        return kernel(
            functools.partial(adam_kernel, at=at, width=width, pieces=pieces, aliased=aliased, **sizes),
            [state] * 3 + [pltpu.VMEM((rows_own, w), bf16) for w in pieces],
            [SM, VM] + [pl.BlockSpec()] * groups + [HB] * (6 if aliased else 3),
            [HB] * 3 + [VM] * len(pieces),
            input_output_aliases={n_in + i: i for i in range(3)} if aliased else {},
            scratch_shapes=[pltpu.VMEM((groups, 8, slots), i32)]
            + [pltpu.VMEM((rows_own, width), jnp.float32)] * 3
            + [pltpu.SemaphoreType.DMA((3,))],
        )(z, near(tokens), *codes, master_rows, first_moment, second_moment, *(map(far, previous) if aliased else ()))

    *new_state, piece_a = adam_part(0, (256,), None)
    *new_state, piece_b, piece_c = adam_part(256, (256, cols - 512), new_state)
    shape = (rows_own, cols * groups)
    got_a, last_a = ring(piece_a, 0, groups)
    got_b, last_b = ring(piece_b, 256, groups)
    got_c, last_c = ring(piece_c, 512, groups)
    half = len(got_a) - 2
    table = put(None, z, got_a[:half] + got_b[:half] + got_c[:half], shape, cols, groups)
    table = put(table, z, got_a[half:] + got_b[half:] + got_c[half:], shape, cols, groups)
    table = put(table, z, last_a + last_b + last_c, shape, cols, groups)
    return (*new_state, table)


def solution(mesh):
    return jax.shard_map(
        step,
        mesh=mesh,
        in_specs=(
            P(("dp", "vocab")),
            P(("dp", "vocab")),
            P(("dp", "vocab"), None),
            P("vocab", "dp"),
            P("vocab", "dp"),
            P("vocab", "dp"),
        ),
        out_specs=(P("vocab", "dp"), P("vocab", "dp"), P("vocab", "dp"), P("vocab", None)),
        check_vma=False,
    )
```

```python
import functools

import jax
import jax.numpy as jnp
from jax import lax
from jax.experimental import pallas as pl
from jax.experimental.pallas import tpu as pltpu
from jax.sharding import PartitionSpec as P


VOCAB = 152064
CAP = 8

beta_one = 0.9
beta_two = 0.999
corr_one = 1.0 - 0.9**10
corr_two = 1.0 - 0.999**10
learn_rate = 0.01
epsilon = 1e-08


def near(x):
    return pltpu.with_memory_space_constraint(x, pltpu.VMEM)


def far(x):
    return pltpu.with_memory_space_constraint(x, pltpu.HBM)


SM = pl.BlockSpec(memory_space=pltpu.SMEM)
VM = pl.BlockSpec(memory_space=pltpu.VMEM)
HB = pl.BlockSpec(memory_space=pltpu.HBM)


def kernel(fn, out_shape, in_specs, out_specs, vmem_limit=24 << 20, **kw):
    def call(*args):
        return pl.pallas_call(
            fn,
            out_shape=out_shape,
            in_specs=in_specs,
            out_specs=out_specs,
            compiler_params=pltpu.CompilerParams(vmem_limit_bytes=vmem_limit),
            **kw,
        )(*args)

    return call


def prep_kernel(count_ref, ids_ref, grads_ref, out_ref, local_ref, buf, obuf, id_buf, sems, out_sems, *, owners, groups, rows_own, cols):
    slots = ids_ref.shape[1]
    into_ids = pltpu.make_async_copy(ids_ref, id_buf, sems.at[groups])
    into_ids.start()
    copies = [pltpu.make_async_copy(grads_ref.at[:, g * cols : (g + 1) * cols], buf.at[g], sems.at[g]) for g in range(groups)]
    for c in copies:
        c.start()
    into_ids.wait()
    first_new = VOCAB - rows_own * owners
    ids = id_buf[...]
    position = lax.broadcasted_iota(jnp.int32, (1, slots), 1)
    live = (position < count_ref[0]) & (ids >= first_new)
    local = jnp.where(live, ids - first_new, -1)
    local_ref[...] = local
    owner = jnp.where(live, local // rows_own, -1)
    key_row = jnp.broadcast_to(owner, (slots, slots))
    key_col = key_row.T
    lane = lax.broadcasted_iota(jnp.int32, (slots, slots), 1)
    sub = lax.broadcasted_iota(jnp.int32, (slots, slots), 0)
    earlier = (key_row == key_col) & (sub < lane)
    rank = jnp.sum(earlier.astype(jnp.int32), axis=0, keepdims=True)
    place = jnp.where(live, owner * CAP + rank, -1)
    placing = (sub == jnp.broadcast_to(place, (slots, slots))).astype(jnp.bfloat16)
    outs = []
    for g in range(groups):
        copies[g].wait()
        got = jnp.dot(placing, buf[g], preferred_element_type=jnp.float32).astype(jnp.bfloat16)
        obuf[g] = got.reshape(owners, CAP, cols)
        out = pltpu.make_async_copy(obuf.at[g], out_ref.at[g * owners : (g + 1) * owners], out_sems.at[g])
        out.start()
        outs.append(out)
    for out in outs:
        out.wait()


def rows_kernel(mine_ref, local_ref, out_ref, *, rows_own):
    owners, slots = local_ref.shape
    mine = mine_ref[0]
    local = local_ref[...]
    here = (local >= mine * rows_own) & (local < (mine + 1) * rows_own)
    row = jnp.where(here, local - mine * rows_own, 0)
    sub = lax.broadcasted_iota(jnp.int32, (slots, slots), 0)
    lane = lax.broadcasted_iota(jnp.int32, (slots, slots), 1)
    ahead = (sub < lane).astype(jnp.bfloat16)
    rank = jnp.dot(here.astype(jnp.bfloat16), ahead, preferred_element_type=jnp.float32)
    lanes = lax.broadcasted_iota(jnp.int32, (owners, slots), 1)
    total = jnp.zeros((owners, slots), jnp.int32)
    for s in range(CAP):
        picked = jnp.where(here & (rank == float(s)), row + 1, 0)
        total = jnp.where(lax.rem(lanes, CAP) == s, jnp.sum(picked, axis=1, keepdims=True), total)
    source = lax.broadcasted_iota(jnp.int32, (owners, slots), 0) ^ mine
    codes = jnp.sum(jnp.where(lanes // CAP == source, total, 0), axis=0, keepdims=True) - 1
    out_ref[...] = jnp.broadcast_to(codes, out_ref.shape)


def adam(gradient, first, second, master):
    new_first = beta_one * first + (1.0 - beta_one) * gradient
    new_second = beta_two * second + (1.0 - beta_two) * gradient * gradient
    update = new_first / corr_one / (jnp.sqrt(new_second / corr_two) + epsilon)
    return new_first, new_second, master - learn_rate * update


def gradient_of(where_ref, tokens_ref, codes, code_buf, owners, groups, rows_own, at, width):
    slots = owners * CAP
    z = where_ref[0]
    for k in range(groups):
        code_buf[lax.rem(z + groups - k, groups)] = codes[k][...]
    sub = lax.broadcasted_iota(jnp.int32, (rows_own, slots), 0)
    gradient = None
    for g in range(groups):
        code = jnp.broadcast_to(code_buf[g, 0:1, :], (rows_own, slots))
        selector = (sub == code).astype(jnp.bfloat16)
        data = tokens_ref[g * owners : (g + 1) * owners, :, at : at + width].reshape(slots, width)
        part = jnp.dot(selector, data, preferred_element_type=jnp.float32)
        gradient = part if gradient is None else gradient + part
    return gradient


def part_of(refs, at, bufs, sems, back=False):
    pairs = [(r.at[:, pl.ds(at, b.shape[1])], b) for r, b in zip(refs, bufs)]
    return [pltpu.make_async_copy(*(p[::-1] if back else p), sems.at[i]) for i, p in enumerate(pairs)]


def adam_one_kernel(where_ref, tokens_ref, *refs, owners, groups, width):
    codes, state, refs = refs[:groups], refs[groups : groups + 3], refs[groups + 3 :]
    om, of, os, piece_ref, code_buf, sems = refs
    into = part_of(state, 0, (om, of, os), sems)
    for c in into:
        c.start()
    gradient = gradient_of(where_ref, tokens_ref, codes, code_buf, owners, groups, om.shape[0], 0, width)
    for c in into:
        c.wait()
    new_first, new_second, new_master = adam(gradient, of[...], os[...], om[...])
    piece_ref[...] = new_master.astype(jnp.bfloat16)
    om[...] = new_master
    of[...] = new_first
    os[...] = new_second


def adam_two_kernel(where_ref, tokens_ref, *refs, owners, groups, at, width, pieces):
    codes, state, early, refs = refs[:groups], refs[groups : groups + 3], refs[groups + 3 : groups + 6], refs[groups + 6 :]
    outs, piece_refs, refs = refs[:3], refs[3 : 3 + len(pieces)], refs[3 + len(pieces) :]
    code_buf, b0, b1, b2, sems, early_sems = refs
    bufs = (b0, b1, b2)
    into = part_of(state, at, bufs, sems)
    over = part_of(outs, 0, early, early_sems, back=True)
    for c in into + over:
        c.start()
    gradient = gradient_of(where_ref, tokens_ref, codes, code_buf, owners, groups, b0.shape[0], at, width)
    for c in into:
        c.wait()
    new_first, new_second, new_master = adam(gradient, b1[...], b2[...], b0[...])
    rounded = new_master.astype(jnp.bfloat16)
    b0[...] = new_master
    b1[...] = new_first
    b2[...] = new_second
    out = part_of(outs, at, bufs, sems, back=True)
    for c in out:
        c.start()
    done = 0
    for piece_ref, w in zip(piece_refs, pieces):
        piece_ref[...] = rounded[:, done : done + w]
        done += w
    for c in over + out:
        c.wait()


def put_kernel(where_ref, *refs, spots, cols, groups, aliased):
    count = len(spots)
    ins = refs[:count]
    table_ref = refs[count + (1 if aliased else 0)]
    sem = refs[-1]
    z = where_ref[0]
    copies = []
    for i, (shift, row, off) in enumerate(spots):
        n, w = ins[i].shape
        g = lax.rem(z + groups - shift, groups)
        at = pl.multiple_of(g * cols + off, 128)
        copies.append(pltpu.make_async_copy(ins[i], table_ref.at[pl.ds(row, n), pl.ds(at, w)], sem.at[i]))
    for c in copies:
        c.start()
    for c in copies:
        c.wait()


def put(table, where, pieces, shape, cols, groups):
    arrays = [near(p[0]) for p in pieces]
    spots = tuple(p[1:] for p in pieces)
    aliased = table is not None
    extra = [far(table)] if aliased else []
    return kernel(
        functools.partial(put_kernel, spots=spots, cols=cols, groups=groups, aliased=aliased),
        jax.ShapeDtypeStruct(shape, jnp.bfloat16),
        [SM] + [VM for _ in arrays] + [HB for _ in extra],
        HB,
        input_output_aliases={len(arrays) + 1: 0} if aliased else {},
        scratch_shapes=[pltpu.SemaphoreType.DMA((len(arrays),))],
    )(where, *arrays, *extra)


def shift_by(x, k, groups):
    return lax.ppermute(x, "dp", [(i, (i + k) % groups) for i in range(groups)])


def ring(piece, off, groups):
    half = groups // 2
    rows = piece.shape[0]
    got = [(piece, 0, 0, off)]
    up = down = piece
    for s in range(1, half):
        up = shift_by(up, 1, groups)
        down = shift_by(down, -1, groups)
        got += [(up, s, 0, off), (down, groups - s, 0, off)]
    last = [
        (shift_by(up[: rows // 2], 1, groups), half, 0, off),
        (shift_by(down[rows // 2 :], -1, groups), half, rows // 2, off),
    ]
    return got, last


def step(token_ids, token_count, out_grads, master_rows, first_moment, second_moment):
    owners = lax.axis_size("vocab")
    groups = lax.axis_size("dp")
    rows_own, cols = master_rows.shape
    slots = token_ids.shape[0]
    bf16, i32 = jnp.bfloat16, jnp.int32
    z = lax.axis_index("dp").astype(i32).reshape(1)
    mine = lax.axis_index("vocab").astype(i32).reshape(1)
    sizes = dict(owners=owners, groups=groups)
    state = jax.ShapeDtypeStruct((rows_own, cols), jnp.float32)
    master_rows, first_moment, second_moment = far(master_rows), far(first_moment), far(second_moment)

    outgoing, local = kernel(
        functools.partial(prep_kernel, rows_own=rows_own, cols=cols, **sizes),
        [pltpu.HBM((groups * owners, CAP, cols), bf16), pltpu.VMEM((1, slots), i32)],
        [SM, HB, HB],
        [HB, VM],
        scratch_shapes=[
            pltpu.VMEM((groups, slots, cols), bf16),
            pltpu.VMEM((groups, owners, CAP, cols), bf16),
            pltpu.VMEM((1, slots), i32),
            pltpu.SemaphoreType.DMA((groups + 1,)),
            pltpu.SemaphoreType.DMA((groups,)),
        ],
    )(token_count, far(token_ids.reshape(1, slots)), far(out_grads))
    tokens = lax.all_to_all(outgoing, ("dp", "vocab"), split_axis=0, concat_axis=0, tiled=True)
    reach = 1
    while reach < owners:
        other = lax.ppermute(local, "vocab", [(i, i ^ reach) for i in range(owners)])
        local = jnp.concatenate([local, other], 0)
        reach *= 2
    codes = kernel(
        functools.partial(rows_kernel, rows_own=rows_own),
        jax.ShapeDtypeStruct((8, slots), i32),
        [SM, pl.BlockSpec()],
        pl.BlockSpec(),
    )(mine, local)
    codes = [codes] + [shift_by(codes, k, groups) for k in range(1, groups)]

    cut = 256
    rest = cols - cut
    f32 = jnp.float32
    *early, piece_a = kernel(
        functools.partial(adam_one_kernel, width=cut, **sizes),
        [pltpu.VMEM((rows_own, cut), f32)] * 3 + [pltpu.VMEM((rows_own, cut), bf16)],
        [SM, VM] + [pl.BlockSpec()] * groups + [HB] * 3,
        [VM] * 4,
        scratch_shapes=[pltpu.VMEM((groups, 8, slots), i32), pltpu.SemaphoreType.DMA((3,))],
    )(z, near(tokens), *codes, master_rows, first_moment, second_moment)
    *new_state, piece_b = kernel(
        functools.partial(adam_two_kernel, at=cut, width=rest, pieces=(rest,), **sizes),
        [state] * 3 + [pltpu.VMEM((rows_own, rest), bf16)],
        [SM, VM] + [pl.BlockSpec()] * groups + [HB] * 3 + [VM] * 3,
        [HB] * 3 + [VM],
        scratch_shapes=[pltpu.VMEM((groups, 8, slots), i32)]
        + [pltpu.VMEM((rows_own, rest), f32)] * 3
        + [pltpu.SemaphoreType.DMA((3,)), pltpu.SemaphoreType.DMA((3,))],
    )(z, near(tokens), *codes, master_rows, first_moment, second_moment, *map(near, early))
    shape = (rows_own, cols * groups)
    got_a, last_a = ring(piece_a, 0, groups)
    got_b, last_b = ring(piece_b, cut, groups)
    half = len(got_a) - 2
    table = put(None, z, got_a[:half] + got_b[:half], shape, cols, groups)
    table = put(table, z, got_a[half:] + got_b[half:], shape, cols, groups)
    table = put(table, z, last_a + last_b, shape, cols, groups)
    return (*new_state, table)


def solution(mesh):
    return jax.shard_map(
        step,
        mesh=mesh,
        in_specs=(
            P(("dp", "vocab")),
            P(("dp", "vocab")),
            P(("dp", "vocab"), None),
            P("vocab", "dp"),
            P("vocab", "dp"),
            P("vocab", "dp"),
        ),
        out_specs=(P("vocab", "dp"), P("vocab", "dp"), P("vocab", "dp"), P("vocab", None)),
        check_vma=False,
    )
```

```python
import functools

import jax
import jax.numpy as jnp
from jax import lax
from jax.experimental import pallas as pl
from jax.experimental.pallas import tpu as pltpu
from jax.sharding import PartitionSpec as P


VOCAB = 152064
CAP = 8

beta_one = 0.9
beta_two = 0.999
corr_one = 1.0 - 0.9**10
corr_two = 1.0 - 0.999**10
learn_rate = 0.01
epsilon = 1e-08


def near(x):
    return pltpu.with_memory_space_constraint(x, pltpu.VMEM)


def far(x):
    return pltpu.with_memory_space_constraint(x, pltpu.HBM)


SM = pl.BlockSpec(memory_space=pltpu.SMEM)
VM = pl.BlockSpec(memory_space=pltpu.VMEM)
HB = pl.BlockSpec(memory_space=pltpu.HBM)


def kernel(fn, out_shape, in_specs, out_specs, vmem_limit=24 << 20, **kw):
    def call(*args):
        return pl.pallas_call(
            fn,
            out_shape=out_shape,
            in_specs=in_specs,
            out_specs=out_specs,
            compiler_params=pltpu.CompilerParams(vmem_limit_bytes=vmem_limit),
            **kw,
        )(*args)

    return call


def prep_kernel(count_ref, ids_ref, grads_ref, out_ref, local_ref, buf, obuf, id_buf, sems, out_sems, *, owners, groups, rows_own, cols):
    slots = ids_ref.shape[1]
    into_ids = pltpu.make_async_copy(ids_ref, id_buf, sems.at[groups])
    into_ids.start()
    wide = buf.shape[2] // cols
    copies = [
        pltpu.make_async_copy(grads_ref.at[:, i * wide * cols : (i + 1) * wide * cols], buf.at[i], sems.at[i]) for i in range(groups // wide)
    ]
    for c in copies:
        c.start()
    into_ids.wait()
    first_new = VOCAB - rows_own * owners
    ids = id_buf[...]
    position = lax.broadcasted_iota(jnp.int32, (1, slots), 1)
    live = (position < count_ref[0]) & (ids >= first_new)
    local = jnp.where(live, ids - first_new, -1)
    local_ref[...] = local
    owner = jnp.where(live, local // rows_own, -1)
    key_row = jnp.broadcast_to(owner, (slots, slots))
    key_col = key_row.T
    lane = lax.broadcasted_iota(jnp.int32, (slots, slots), 1)
    sub = lax.broadcasted_iota(jnp.int32, (slots, slots), 0)
    earlier = (key_row == key_col) & (sub < lane)
    rank = jnp.sum(earlier.astype(jnp.int32), axis=0, keepdims=True)
    place = jnp.where(live, owner * CAP + rank, -1)
    placing = (sub == jnp.broadcast_to(place, (slots, slots))).astype(jnp.bfloat16)
    outs = []
    for i in range(groups // wide):
        copies[i].wait()
        got = jnp.dot(placing, buf[i], preferred_element_type=jnp.float32).astype(jnp.bfloat16)
        for g in range(i * wide, (i + 1) * wide):
            part = got[:, (g - i * wide) * cols : (g - i * wide + 1) * cols]
            obuf[g] = part.reshape(owners, CAP, cols)
            out = pltpu.make_async_copy(obuf.at[g], out_ref.at[g * owners : (g + 1) * owners], out_sems.at[g])
            out.start()
            outs.append(out)
    for out in outs:
        out.wait()


def rows_kernel(mine_ref, local_ref, out_ref, *, rows_own):
    owners, slots = local_ref.shape
    mine = mine_ref[0]
    local = local_ref[...]
    here = (local >= mine * rows_own) & (local < (mine + 1) * rows_own)
    row = jnp.where(here, local - mine * rows_own, 0)
    sub = lax.broadcasted_iota(jnp.int32, (slots, slots), 0)
    lane = lax.broadcasted_iota(jnp.int32, (slots, slots), 1)
    ahead = (sub < lane).astype(jnp.bfloat16)
    rank = jnp.dot(here.astype(jnp.bfloat16), ahead, preferred_element_type=jnp.float32)
    lanes = lax.broadcasted_iota(jnp.int32, (owners, slots), 1)
    total = jnp.zeros((owners, slots), jnp.int32)
    for s in range(CAP):
        picked = jnp.where(here & (rank == float(s)), row + 1, 0)
        total = jnp.where(lax.rem(lanes, CAP) == s, jnp.sum(picked, axis=1, keepdims=True), total)
    source = lax.broadcasted_iota(jnp.int32, (owners, slots), 0) ^ mine
    codes = jnp.sum(jnp.where(lanes // CAP == source, total, 0), axis=0, keepdims=True) - 1
    out_ref[...] = jnp.broadcast_to(codes, out_ref.shape)


def adam(gradient, first, second, master):
    new_first = beta_one * first + (1.0 - beta_one) * gradient
    new_second = beta_two * second + (1.0 - beta_two) * gradient * gradient
    update = new_first / corr_one / (jnp.sqrt(new_second / corr_two) + epsilon)
    return new_first, new_second, master - learn_rate * update


def gradient_of(where_ref, tokens_ref, codes, code_buf, owners, groups, rows_own, at, width):
    slots = owners * CAP
    z = where_ref[0]
    for k in range(groups):
        code_buf[lax.rem(z + groups - k, groups)] = codes[k][...]
    sub = lax.broadcasted_iota(jnp.int32, (rows_own, slots), 0)
    gradient = None
    for g in range(groups):
        code = jnp.broadcast_to(code_buf[g, 0:1, :], (rows_own, slots))
        selector = (sub == code).astype(jnp.bfloat16)
        data = tokens_ref[g * owners : (g + 1) * owners, :, at : at + width].reshape(slots, width)
        part = jnp.dot(selector, data, preferred_element_type=jnp.float32)
        gradient = part if gradient is None else gradient + part
    return gradient


def part_of(refs, at, bufs, sems, back=False):
    pairs = [(r.at[:, pl.ds(at, b.shape[1])], b) for r, b in zip(refs, bufs)]
    return [pltpu.make_async_copy(*(p[::-1] if back else p), sems.at[i]) for i, p in enumerate(pairs)]


def adam_one_kernel(where_ref, tokens_ref, *refs, owners, groups, width):
    codes, state, refs = refs[:groups], refs[groups : groups + 3], refs[groups + 3 :]
    om, of, os, piece_ref, code_buf, sems = refs
    into = part_of(state, 0, (om, of, os), sems)
    for c in into:
        c.start()
    gradient = gradient_of(where_ref, tokens_ref, codes, code_buf, owners, groups, om.shape[0], 0, width)
    for c in into:
        c.wait()
    new_first, new_second, new_master = adam(gradient, of[...], os[...], om[...])
    piece_ref[...] = new_master.astype(jnp.bfloat16)
    om[...] = new_master
    of[...] = new_first
    os[...] = new_second


def adam_two_kernel(where_ref, tokens_ref, *refs, owners, groups, at, width, pieces):
    codes, state, early, refs = refs[:groups], refs[groups : groups + 3], refs[groups + 3 : groups + 6], refs[groups + 6 :]
    outs, piece_refs, refs = refs[:3], refs[3 : 3 + len(pieces)], refs[3 + len(pieces) :]
    code_buf, b0, b1, b2, sems, early_sems = refs
    bufs = (b0, b1, b2)
    into = part_of(state, at, bufs, sems)
    over = part_of(outs, 0, early, early_sems, back=True)
    for c in into + over:
        c.start()
    gradient = gradient_of(where_ref, tokens_ref, codes, code_buf, owners, groups, b0.shape[0], at, width)
    for c in into:
        c.wait()
    new_first, new_second, new_master = adam(gradient, b1[...], b2[...], b0[...])
    rounded = new_master.astype(jnp.bfloat16)
    b0[...] = new_master
    b1[...] = new_first
    b2[...] = new_second
    out = part_of(outs, at, bufs, sems, back=True)
    for c in out:
        c.start()
    done = 0
    for piece_ref, w in zip(piece_refs, pieces):
        piece_ref[...] = rounded[:, done : done + w]
        done += w
    for c in over + out:
        c.wait()


def put_kernel(where_ref, *refs, spots, cols, groups, aliased):
    count = len(spots)
    ins = refs[:count]
    table_ref = refs[count + (1 if aliased else 0)]
    sem = refs[-1]
    z = where_ref[0]
    copies = []
    for i, (shift, row, off) in enumerate(spots):
        n, w = ins[i].shape
        g = lax.rem(z + groups - shift, groups)
        at = pl.multiple_of(g * cols + off, 128)
        copies.append(pltpu.make_async_copy(ins[i], table_ref.at[pl.ds(row, n), pl.ds(at, w)], sem.at[i]))
    for c in copies:
        c.start()
    for c in copies:
        c.wait()


def put(table, where, pieces, shape, cols, groups):
    arrays = [near(p[0]) for p in pieces]
    spots = tuple(p[1:] for p in pieces)
    aliased = table is not None
    extra = [far(table)] if aliased else []
    return kernel(
        functools.partial(put_kernel, spots=spots, cols=cols, groups=groups, aliased=aliased),
        jax.ShapeDtypeStruct(shape, jnp.bfloat16),
        [SM] + [VM for _ in arrays] + [HB for _ in extra],
        HB,
        input_output_aliases={len(arrays) + 1: 0} if aliased else {},
        scratch_shapes=[pltpu.SemaphoreType.DMA((len(arrays),))],
    )(where, *arrays, *extra)


def shift_by(x, k, groups):
    return lax.ppermute(x, "dp", [(i, (i + k) % groups) for i in range(groups)])


def ring(piece, off, groups):
    half = groups // 2
    rows = piece.shape[0]
    got = [(piece, 0, 0, off)]
    up = down = piece
    for s in range(1, half):
        up = shift_by(up, 1, groups)
        down = shift_by(down, -1, groups)
        got += [(up, s, 0, off), (down, groups - s, 0, off)]
    last = [
        (shift_by(up[: rows // 2], 1, groups), half, 0, off),
        (shift_by(down[rows // 2 :], -1, groups), half, rows // 2, off),
    ]
    return got, last


def step(token_ids, token_count, out_grads, master_rows, first_moment, second_moment):
    owners = lax.axis_size("vocab")
    groups = lax.axis_size("dp")
    rows_own, cols = master_rows.shape
    slots = token_ids.shape[0]
    bf16, i32 = jnp.bfloat16, jnp.int32
    z = lax.axis_index("dp").astype(i32).reshape(1)
    mine = lax.axis_index("vocab").astype(i32).reshape(1)
    sizes = dict(owners=owners, groups=groups)
    state = jax.ShapeDtypeStruct((rows_own, cols), jnp.float32)
    master_rows, first_moment, second_moment = far(master_rows), far(first_moment), far(second_moment)

    outgoing, local = kernel(
        functools.partial(prep_kernel, rows_own=rows_own, cols=cols, **sizes),
        [pltpu.HBM((groups * owners, CAP, cols), bf16), pltpu.VMEM((1, slots), i32)],
        [SM, HB, HB],
        [HB, VM],
        scratch_shapes=[
            pltpu.VMEM((groups // 2, slots, 2 * cols), bf16),
            pltpu.VMEM((groups, owners, CAP, cols), bf16),
            pltpu.VMEM((1, slots), i32),
            pltpu.SemaphoreType.DMA((groups + 1,)),
            pltpu.SemaphoreType.DMA((groups,)),
        ],
    )(token_count, far(token_ids.reshape(1, slots)), far(out_grads))
    tokens = lax.all_to_all(outgoing, ("dp", "vocab"), split_axis=0, concat_axis=0, tiled=True)
    reach = 1
    while reach < owners:
        other = lax.ppermute(local, "vocab", [(i, i ^ reach) for i in range(owners)])
        local = jnp.concatenate([local, other], 0)
        reach *= 2
    codes = kernel(
        functools.partial(rows_kernel, rows_own=rows_own),
        jax.ShapeDtypeStruct((8, slots), i32),
        [SM, pl.BlockSpec()],
        pl.BlockSpec(),
    )(mine, local)
    codes = [codes] + [shift_by(codes, k, groups) for k in range(1, groups)]

    cut = 384
    rest = cols - cut
    f32 = jnp.float32
    *early, piece_a = kernel(
        functools.partial(adam_one_kernel, width=cut, **sizes),
        [pltpu.VMEM((rows_own, cut), f32)] * 3 + [pltpu.VMEM((rows_own, cut), bf16)],
        [SM, VM] + [pl.BlockSpec()] * groups + [HB] * 3,
        [VM] * 4,
        scratch_shapes=[pltpu.VMEM((groups, 8, slots), i32), pltpu.SemaphoreType.DMA((3,))],
    )(z, near(tokens), *codes, master_rows, first_moment, second_moment)
    *new_state, piece_b = kernel(
        functools.partial(adam_two_kernel, at=cut, width=rest, pieces=(rest,), **sizes),
        [state] * 3 + [pltpu.VMEM((rows_own, rest), bf16)],
        [SM, VM] + [pl.BlockSpec()] * groups + [HB] * 3 + [VM] * 3,
        [HB] * 3 + [VM],
        scratch_shapes=[pltpu.VMEM((groups, 8, slots), i32)]
        + [pltpu.VMEM((rows_own, rest), f32)] * 3
        + [pltpu.SemaphoreType.DMA((3,)), pltpu.SemaphoreType.DMA((3,))],
    )(z, near(tokens), *codes, master_rows, first_moment, second_moment, *map(near, early))
    shape = (rows_own, cols * groups)
    got_a, last_a = ring(piece_a, 0, groups)
    got_b, last_b = ring(piece_b, cut, groups)
    half = len(got_a) - 2
    table = put(None, z, got_a[:half] + got_b[:half], shape, cols, groups)
    table = put(table, z, got_a[half:] + got_b[half:], shape, cols, groups)
    table = put(table, z, last_a, shape, cols, groups)
    table = put(table, z, last_b, shape, cols, groups)
    return (*new_state, table)


def solution(mesh):
    return jax.shard_map(
        step,
        mesh=mesh,
        in_specs=(
            P(("dp", "vocab")),
            P(("dp", "vocab")),
            P(("dp", "vocab"), None),
            P("vocab", "dp"),
            P("vocab", "dp"),
            P("vocab", "dp"),
        ),
        out_specs=(P("vocab", "dp"), P("vocab", "dp"), P("vocab", "dp"), P("vocab", None)),
        check_vma=False,
    )
```

```python
import functools

import jax
import jax.numpy as jnp
from jax import lax
from jax.experimental import pallas as pl
from jax.experimental.pallas import tpu as pltpu
from jax.sharding import PartitionSpec as P


VOCAB = 152064
CAP = 8

beta_one = 0.9
beta_two = 0.999
corr_one = 1.0 - 0.9**10
corr_two = 1.0 - 0.999**10
learn_rate = 0.01
epsilon = 1e-08


def near(x):
    return pltpu.with_memory_space_constraint(x, pltpu.VMEM)


def far(x):
    return pltpu.with_memory_space_constraint(x, pltpu.HBM)


SM = pl.BlockSpec(memory_space=pltpu.SMEM)
VM = pl.BlockSpec(memory_space=pltpu.VMEM)
HB = pl.BlockSpec(memory_space=pltpu.HBM)


def kernel(fn, out_shape, in_specs, out_specs, vmem_limit=24 << 20, **kw):
    def call(*args):
        return pl.pallas_call(
            fn,
            out_shape=out_shape,
            in_specs=in_specs,
            out_specs=out_specs,
            compiler_params=pltpu.CompilerParams(vmem_limit_bytes=vmem_limit),
            **kw,
        )(*args)

    return call


def prep_kernel(count_ref, ids_ref, grads_ref, out_ref, local_ref, buf, obuf, id_buf, sems, out_sems, *, owners, groups, rows_own, cols):
    slots = ids_ref.shape[1]
    into_ids = pltpu.make_async_copy(ids_ref, id_buf, sems.at[groups])
    into_ids.start()
    wide = buf.shape[2] // cols
    copies = [
        pltpu.make_async_copy(grads_ref.at[:, i * wide * cols : (i + 1) * wide * cols], buf.at[i], sems.at[i]) for i in range(groups // wide)
    ]
    for c in copies:
        c.start()
    into_ids.wait()
    first_new = VOCAB - rows_own * owners
    ids = id_buf[...]
    position = lax.broadcasted_iota(jnp.int32, (1, slots), 1)
    live = (position < count_ref[0]) & (ids >= first_new)
    local = jnp.where(live, ids - first_new, -1)
    local_ref[...] = local
    owner = jnp.where(live, local // rows_own, -1)
    key_row = jnp.broadcast_to(owner, (slots, slots))
    key_col = key_row.T
    lane = lax.broadcasted_iota(jnp.int32, (slots, slots), 1)
    sub = lax.broadcasted_iota(jnp.int32, (slots, slots), 0)
    earlier = (key_row == key_col) & (sub < lane)
    rank = jnp.sum(earlier.astype(jnp.int32), axis=0, keepdims=True)
    place = jnp.where(live, owner * CAP + rank, -1)
    placing = (sub == jnp.broadcast_to(place, (slots, slots))).astype(jnp.bfloat16)
    outs = []
    for i in range(groups // wide):
        copies[i].wait()
        got = jnp.dot(placing, buf[i], preferred_element_type=jnp.float32).astype(jnp.bfloat16)
        for g in range(i * wide, (i + 1) * wide):
            part = got[:, (g - i * wide) * cols : (g - i * wide + 1) * cols]
            obuf[g] = part.reshape(owners, CAP, cols)
            out = pltpu.make_async_copy(obuf.at[g], out_ref.at[g * owners : (g + 1) * owners], out_sems.at[g])
            out.start()
            outs.append(out)
    for out in outs:
        out.wait()


def rows_kernel(mine_ref, local_ref, out_ref, *, rows_own):
    owners, slots = local_ref.shape
    mine = mine_ref[0]
    local = local_ref[...]
    here = (local >= mine * rows_own) & (local < (mine + 1) * rows_own)
    row = jnp.where(here, local - mine * rows_own, 0)
    sub = lax.broadcasted_iota(jnp.int32, (slots, slots), 0)
    lane = lax.broadcasted_iota(jnp.int32, (slots, slots), 1)
    ahead = (sub < lane).astype(jnp.bfloat16)
    rank = jnp.dot(here.astype(jnp.bfloat16), ahead, preferred_element_type=jnp.float32)
    lanes = lax.broadcasted_iota(jnp.int32, (owners, slots), 1)
    total = jnp.zeros((owners, slots), jnp.int32)
    for s in range(CAP):
        picked = jnp.where(here & (rank == float(s)), row + 1, 0)
        total = jnp.where(lax.rem(lanes, CAP) == s, jnp.sum(picked, axis=1, keepdims=True), total)
    source = lax.broadcasted_iota(jnp.int32, (owners, slots), 0) ^ mine
    codes = jnp.sum(jnp.where(lanes // CAP == source, total, 0), axis=0, keepdims=True) - 1
    out_ref[...] = jnp.broadcast_to(codes, out_ref.shape)


def adam(gradient, first, second, master):
    new_first = beta_one * first + (1.0 - beta_one) * gradient
    new_second = beta_two * second + (1.0 - beta_two) * gradient * gradient
    update = new_first / corr_one / (jnp.sqrt(new_second / corr_two) + epsilon)
    return new_first, new_second, master - learn_rate * update


def gradient_of(where_ref, tokens_ref, codes, code_buf, owners, groups, rows, at):
    slots = owners * CAP
    z = where_ref[0]
    for k in range(groups):
        code_buf[lax.rem(z + groups - k, groups)] = codes[k][...]
    width = tokens_ref.shape[2]
    sub = lax.broadcasted_iota(jnp.int32, (rows, slots), 0) + at
    gradient = None
    for g in range(groups):
        code = jnp.broadcast_to(code_buf[g, 0:1, :], (rows, slots))
        selector = (sub == code).astype(jnp.bfloat16)
        data = tokens_ref[g * owners : (g + 1) * owners].reshape(slots, width)
        part = jnp.dot(selector, data, preferred_element_type=jnp.float32)
        gradient = part if gradient is None else gradient + part
    return gradient


def part_of(refs, at, bufs, sems, back=False):
    pairs = [(r.at[pl.ds(at, b.shape[0])], b) for r, b in zip(refs, bufs)]
    return [pltpu.make_async_copy(*(p[::-1] if back else p), sems.at[i]) for i, p in enumerate(pairs)]


def adam_one_kernel(where_ref, tokens_ref, *refs, owners, groups):
    codes, state, refs = refs[:groups], refs[groups : groups + 3], refs[groups + 3 :]
    om, of, os, piece_ref, code_buf, sems = refs
    into = part_of(state, 0, (om, of, os), sems)
    for c in into:
        c.start()
    gradient = gradient_of(where_ref, tokens_ref, codes, code_buf, owners, groups, om.shape[0], 0)
    for c in into:
        c.wait()
    new_first, new_second, new_master = adam(gradient, of[...], os[...], om[...])
    piece_ref[...] = new_master.astype(jnp.bfloat16)
    om[...] = new_master
    of[...] = new_first
    os[...] = new_second


def adam_two_kernel(where_ref, tokens_ref, *refs, owners, groups, at):
    codes, state, early, refs = refs[:groups], refs[groups : groups + 3], refs[groups + 3 : groups + 6], refs[groups + 6 :]
    outs, piece_ref, refs = refs[:3], refs[3], refs[4:]
    code_buf, b0, b1, b2, sems, early_sems = refs
    bufs = (b0, b1, b2)
    into = part_of(state, at, bufs, sems)
    over = part_of(outs, 0, early, early_sems, back=True)
    for c in into + over:
        c.start()
    gradient = gradient_of(where_ref, tokens_ref, codes, code_buf, owners, groups, b0.shape[0], at)
    for c in into:
        c.wait()
    new_first, new_second, new_master = adam(gradient, b1[...], b2[...], b0[...])
    rounded = new_master.astype(jnp.bfloat16)
    b0[...] = new_master
    b1[...] = new_first
    b2[...] = new_second
    out = part_of(outs, at, bufs, sems, back=True)
    for c in out:
        c.start()
    piece_ref[...] = rounded
    for c in over + out:
        c.wait()


def put_kernel(where_ref, *refs, spots, cols, groups, aliased):
    count = len(spots)
    ins = refs[:count]
    table_ref = refs[count + (1 if aliased else 0)]
    sem = refs[-1]
    z = where_ref[0]
    copies = []
    for i, (shift, row, off) in enumerate(spots):
        n, w = ins[i].shape
        g = lax.rem(z + groups - shift, groups)
        at = pl.multiple_of(g * cols + off, 128)
        copies.append(pltpu.make_async_copy(ins[i], table_ref.at[pl.ds(row, n), pl.ds(at, w)], sem.at[i]))
    for c in copies:
        c.start()
    for c in copies:
        c.wait()


def put(table, where, pieces, shape, cols, groups):
    arrays = [near(p[0]) for p in pieces]
    spots = tuple(p[1:] for p in pieces)
    aliased = table is not None
    extra = [far(table)] if aliased else []
    return kernel(
        functools.partial(put_kernel, spots=spots, cols=cols, groups=groups, aliased=aliased),
        jax.ShapeDtypeStruct(shape, jnp.bfloat16),
        [SM] + [VM for _ in arrays] + [HB for _ in extra],
        HB,
        input_output_aliases={len(arrays) + 1: 0} if aliased else {},
        scratch_shapes=[pltpu.SemaphoreType.DMA((len(arrays),))],
    )(where, *arrays, *extra)


def shift_by(x, k, groups):
    return lax.ppermute(x, "dp", [(i, (i + k) % groups) for i in range(groups)])


def ring(piece, row, groups):
    half = groups // 2
    rows = piece.shape[0]
    got = [(piece, 0, row, 0)]
    up = down = piece
    for s in range(1, half):
        up = shift_by(up, 1, groups)
        down = shift_by(down, -1, groups)
        got += [(up, s, row, 0), (down, groups - s, row, 0)]
    last = [
        (shift_by(up[: rows // 2], 1, groups), half, row, 0),
        (shift_by(down[rows // 2 :], -1, groups), half, row + rows // 2, 0),
    ]
    return got, last


def step(token_ids, token_count, out_grads, master_rows, first_moment, second_moment):
    owners = lax.axis_size("vocab")
    groups = lax.axis_size("dp")
    rows_own, cols = master_rows.shape
    slots = token_ids.shape[0]
    bf16, i32 = jnp.bfloat16, jnp.int32
    z = lax.axis_index("dp").astype(i32).reshape(1)
    mine = lax.axis_index("vocab").astype(i32).reshape(1)
    sizes = dict(owners=owners, groups=groups)
    state = jax.ShapeDtypeStruct((rows_own, cols), jnp.float32)
    master_rows, first_moment, second_moment = far(master_rows), far(first_moment), far(second_moment)

    outgoing, local = kernel(
        functools.partial(prep_kernel, rows_own=rows_own, cols=cols, **sizes),
        [pltpu.HBM((groups * owners, CAP, cols), bf16), pltpu.VMEM((1, slots), i32)],
        [SM, HB, HB],
        [HB, VM],
        scratch_shapes=[
            pltpu.VMEM((groups // 4, slots, 4 * cols), bf16),
            pltpu.VMEM((groups, owners, CAP, cols), bf16),
            pltpu.VMEM((1, slots), i32),
            pltpu.SemaphoreType.DMA((groups + 1,)),
            pltpu.SemaphoreType.DMA((groups,)),
        ],
    )(token_count, far(token_ids.reshape(1, slots)), far(out_grads))
    tokens = lax.all_to_all(outgoing, ("dp", "vocab"), split_axis=0, concat_axis=0, tiled=True)
    reach = 1
    while reach < owners:
        other = lax.ppermute(local, "vocab", [(i, i ^ reach) for i in range(owners)])
        local = jnp.concatenate([local, other], 0)
        reach *= 2
    codes = kernel(
        functools.partial(rows_kernel, rows_own=rows_own),
        jax.ShapeDtypeStruct((8, slots), i32),
        [SM, pl.BlockSpec()],
        pl.BlockSpec(),
    )(mine, local)
    codes = [codes] + [shift_by(codes, k, groups) for k in range(1, groups)]

    cut = 304
    rest = rows_own - cut
    f32 = jnp.float32
    *early, piece_a = kernel(
        functools.partial(adam_one_kernel, **sizes),
        [pltpu.VMEM((cut, cols), f32)] * 3 + [pltpu.VMEM((cut, cols), bf16)],
        [SM, VM] + [pl.BlockSpec()] * groups + [HB] * 3,
        [VM] * 4,
        scratch_shapes=[pltpu.VMEM((groups, 8, slots), i32), pltpu.SemaphoreType.DMA((3,))],
    )(z, near(tokens), *codes, master_rows, first_moment, second_moment)
    *new_state, piece_b = kernel(
        functools.partial(adam_two_kernel, at=cut, **sizes),
        [state] * 3 + [pltpu.VMEM((rest, cols), bf16)],
        [SM, VM] + [pl.BlockSpec()] * groups + [HB] * 3 + [VM] * 3,
        [HB] * 3 + [VM],
        scratch_shapes=[pltpu.VMEM((groups, 8, slots), i32)]
        + [pltpu.VMEM((rest, cols), f32)] * 3
        + [pltpu.SemaphoreType.DMA((3,)), pltpu.SemaphoreType.DMA((3,))],
    )(z, near(tokens), *codes, master_rows, first_moment, second_moment, *map(near, early))
    shape = (rows_own, cols * groups)
    got_a, last_a = ring(piece_a, 0, groups)
    got_b, last_b = ring(piece_b, cut, groups)
    half = len(got_a) - 2
    table = put(None, z, got_a[:half] + got_b[:half], shape, cols, groups)
    table = put(table, z, got_a[half:] + got_b[half:], shape, cols, groups)
    table = put(table, z, last_a, shape, cols, groups)
    table = put(table, z, last_b, shape, cols, groups)
    return (*new_state, table)


def solution(mesh):
    return jax.shard_map(
        step,
        mesh=mesh,
        in_specs=(
            P(("dp", "vocab")),
            P(("dp", "vocab")),
            P(("dp", "vocab"), None),
            P("vocab", "dp"),
            P("vocab", "dp"),
            P("vocab", "dp"),
        ),
        out_specs=(P("vocab", "dp"), P("vocab", "dp"), P("vocab", "dp"), P("vocab", None)),
        check_vma=False,
    )
```
